32 devices in a mesh: src: 8 (over z, x), tgt: 4 (over y, core).
Axes of the slice: x: 2, y: 2, z: 4, core: 2. Of those that a mesh axis runs over, the one named last changes fastest.
Arguments:
- sources: bfloat16 [65536, 64], P(('src', 'tgt')), may hold values from -2.09375 to 2.09375
- targets: bfloat16 [65536, 64], P('tgt'), may hold values from -2.09375 to 2.09375
- potential: float32 [65536], P('src'), may hold values from -1 to 112
- block_map: int32 [256, 20], P('src'), may hold values from -1 to 255, as said below
- counts: int32 [256], P('src'), may hold values from 10 to 20, as said below
- step_history: float32 [8, 65536], P(None, ('src', 'tgt')), may hold values from -13 to 13
- slope_history: float32 [8, 65536], P(None, ('src', 'tgt')), may hold values from -64 to 64, as said below
Outputs:
- gradient: float32 [65536], P(('src', 'tgt'))
- direction: float32 [65536], P(('src', 'tgt'))
- target_potential: float32 [65536], P('tgt')
The draws below stay inside these ranges and needn't reach their ends.
Inputs may be any that keep to these rules, and one draw needn't show every extreme that they name: `block_map`: row b lists counts[b] different target block numbers in slots 0 to counts[b] - 1 and -1 in the other slots; every target block is listed in some row. `counts`: some source block lists exactly 20 target blocks in every draw. For every k the sum over all points of step_history[k] slope_history[k] is positive.
All inputs are finite; a program needn't handle non-finite values.
Results may differ from the reference program's by a relative error of at most 0.0008.
Values may be sent and summed in bfloat16 or wider, within the bound.
A program may use at most 64 MiB of HBM per device.

```python
import jax
import jax.numpy as jnp
from jax import lax

D = 64
BLOCK = 256
KMAX = 20
HIST = 8
NSB = 256
NTB = 256
NS = 65536
NT = 65536


def block_layout(key):
    seeded = jax.random.fold_in(key, 101)
    key_count, key_first, key_second, key_mixing, key_shuffle = jax.random.split(seeded, 5)
    lowest = max(KMAX // 2, 1)
    block_index = jnp.arange(NSB, dtype=jnp.int32)
    number = jax.random.randint(key_count, (NSB,), lowest, KMAX + 1)
    number = jnp.where(block_index == 0, KMAX, number)
    first_draw = jax.random.randint(key_first, (NSB,), 0, NTB)
    second_draw = jax.random.randint(key_second, (NSB,), 0, NTB)
    mixing = jax.random.randint(key_mixing, (NSB,), 0, 2)
    center = jnp.where(mixing == 1, first_draw * second_draw // NTB, first_draw)
    window = 2 * KMAX
    spacing = max(NTB // window, 1)
    offsets = jnp.arange(window, dtype=jnp.int32) - KMAX
    candidate = (center[:, None] + offsets[None, :] * spacing) % NTB
    homeward = block_index % NTB
    ranking = jax.random.randint(key_shuffle, (NSB, window), 0, 2 ** 20) * window + offsets[None, :] + KMAX
    ranking = jnp.where(candidate == homeward[:, None], 2 ** 30, ranking)
    ordering = jnp.argsort(ranking, axis=1)
    others = jnp.take_along_axis(candidate, ordering, axis=1)[:, :KMAX - 1]
    listing = jnp.concatenate([homeward[:, None], others], axis=1)
    slot_index = jnp.arange(KMAX, dtype=jnp.int32)
    listing = jnp.where(slot_index[None, :] < number[:, None], listing, -1)
    return (listing.astype(jnp.int32), number.astype(jnp.int32))


def draw_block_map(key, part):
    return block_layout(key)[0]


def draw_counts(key, part):
    return block_layout(key)[1]


def draw_potential(key, part):
    seeded = jax.random.fold_in(key, 303)
    key_noise = jax.random.fold_in(seeded, 0)
    point_index = jnp.arange(NS, dtype=jnp.int32)
    ramp_term = jnp.log(1.0 + 2.0 * point_index.astype(jnp.float32) / (NS - 1))
    noise = 0.5 * jnp.clip(jax.random.normal(key_noise, (NS,), jnp.float32), -3.0, 3.0)
    values = 0.5 * (noise + ramp_term)
    return values.astype(jnp.float32)


def history_pair(key):
    seeded = jax.random.fold_in(key, 202)
    key_steps, key_factor = jax.random.split(seeded, 2)
    point_index = jnp.arange(NS, dtype=jnp.int32).astype(jnp.float32)
    ramp_term = 1.0 + 2.0 * point_index / (NS - 1)
    steps_drawn = 0.5 * ramp_term[None, :] * jnp.clip(jax.random.normal(key_steps, (HIST, NS), jnp.float32), -4.0, 4.0)
    factor = jnp.exp(jax.random.uniform(key_factor, (HIST, NS), jnp.float32, jnp.log(0.3), jnp.log(3.0)))
    return (steps_drawn, steps_drawn * factor)


def draw_step_history(key, part):
    return history_pair(key)[0].astype(jnp.float32)


def draw_slope_history(key, part):
    return history_pair(key)[1].astype(jnp.float32)


def steps_of(rng, extent, cuts, least, top_value):
    level, own = 1.0, jax.random.fold_in(rng, 6)
    for position, shards_of in cuts:
        draws = jnp.exp(jax.random.uniform(jax.random.fold_in(own, position), (shards_of,), jnp.float32, least / len(cuts), top_value / len(cuts)))
        level = level * jnp.repeat(draws, extent[position] // shards_of).reshape([-1 if axis == position else 1 for axis in range(len(extent))])
    return level


def gaussian(stream_key, extent, deviation, bound, pieces=(), held_as=jnp.bfloat16):
    loudness = steps_of(stream_key, extent, pieces, -0.22, 0.18) if pieces else 1.0
    values = jax.random.normal(stream_key, extent, jnp.float32) * deviation * loudness
    return jnp.minimum(jnp.maximum(values, -bound), bound).astype(held_as)


def setup_inputs(seed: int = 0) -> dict:
    key_of = jax.random.split(jax.random.key(seed), 8)
    return {
        "sources": gaussian(key_of[0], (NS, D), 0.35, 2.09375, ((0, 32),)),
        "targets": gaussian(key_of[1], (NT, D), 0.35, 2.09375, ((0, 4),)),
        "potential": draw_potential(jax.random.fold_in(key_of[7], 71), 0),
        "block_map": draw_block_map(jax.random.fold_in(key_of[7], 71), 0),
        "counts": draw_counts(jax.random.fold_in(key_of[7], 71), 0),
        "step_history": draw_step_history(jax.random.fold_in(key_of[7], 71), 0),
        "slope_history": draw_slope_history(jax.random.fold_in(key_of[7], 71), 0),
    }


entropy = 0.5


def block_scores(source_tiles, potential_tiles, target_tiles, block_map, counts, block):
    slot_index = jnp.arange(KMAX, dtype=jnp.int32)
    live = slot_index < counts[block]
    safe = jnp.where(live, block_map[block], 0).astype(jnp.int32)
    tiles = target_tiles[safe].astype(jnp.float32)
    rows_in = source_tiles[block].astype(jnp.float32)
    product = jnp.einsum("id,kjd->kij", rows_in, tiles)
    return (potential_tiles[block][None, :, None] + product) / entropy, live, safe


def reference(sources, targets, potential, block_map, counts, step_history, slope_history):
    source_tiles = sources.reshape(NSB, BLOCK, D)
    target_tiles = targets.reshape(NTB, BLOCK, D)
    potential_tiles = potential.reshape(NSB, BLOCK)
    blocks_all = jnp.arange(NSB, dtype=jnp.int32)

    def column_step(carry, block):
        peak, total = carry
        scores, live, safe = block_scores(source_tiles, potential_tiles, target_tiles, block_map, counts, block)
        tile_peak = jnp.max(scores, axis=1)
        tile_total = jnp.sum(jnp.exp(scores - tile_peak[:, None, :]), axis=1)
        target_ids = jnp.where(live, safe, NTB).astype(jnp.int32)
        old_peak = peak[target_ids]
        new_peak = jnp.maximum(old_peak, tile_peak)
        new_total = total[target_ids] * jnp.exp(old_peak - new_peak) + tile_total * jnp.exp(tile_peak - new_peak)
        return (peak.at[target_ids].set(new_peak), total.at[target_ids].set(new_total)), None

    start_peak = jnp.full((NTB + 1, BLOCK), -1e30, jnp.float32)
    start_total = jnp.zeros((NTB + 1, BLOCK), jnp.float32)
    (peak, total), _ = lax.scan(column_step, (start_peak, start_total), blocks_all)
    log_tiles = peak[:NTB] + jnp.log(total[:NTB])
    target_potential = -entropy * log_tiles.reshape(NT)

    def row_step(carry, block):
        scores, live, safe = block_scores(source_tiles, potential_tiles, target_tiles, block_map, counts, block)
        weights = jnp.exp(scores - log_tiles[safe][:, None, :])
        weights = jnp.where(live[:, None, None], weights, 0.0)
        return carry, jnp.sum(weights, axis=(0, 2))

    _, masses = lax.scan(row_step, 0.0, blocks_all)
    gradient = 1.0 - (NS / NT) * masses.reshape(NS)

    inverse = []
    for index in range(HIST):
        inverse.append(1.0 / jnp.sum(step_history[index] * slope_history[index]))
    scale = jnp.sum(step_history[HIST - 1] * slope_history[HIST - 1]) / jnp.sum(slope_history[HIST - 1] * slope_history[HIST - 1])
    search = gradient
    alphas = [None] * HIST
    for index in reversed(range(HIST)):
        alphas[index] = inverse[index] * jnp.sum(step_history[index] * search)
        search = search - alphas[index] * slope_history[index]
    result = scale * search
    for index in range(HIST):
        beta_value = inverse[index] * jnp.sum(slope_history[index] * result)
        result = result + (alphas[index] - beta_value) * step_history[index]
    direction = -result
    return gradient, direction, target_potential
```

```python
import functools
import math

import jax
import jax.numpy as jnp
from jax import lax
from jax.experimental import pallas as pl
from jax.experimental.pallas import tpu as pltpu
from jax.sharding import PartitionSpec as P

BLOCK = 256
LANES = 128
UNROLL = 4
FLOOR = -1e30

entropy = 0.5
exponent = math.log2(math.e) / entropy


def pieces(value):
    high = lax.reduce_precision(value, 8, 7)
    middle = lax.reduce_precision(value - high, 8, 7)
    low = lax.reduce_precision(value - high - middle, 8, 7)
    return high, middle, low


def kernel_pieces(value):
    high = value.astype(jnp.bfloat16).astype(jnp.float32)
    middle = (value - high).astype(jnp.bfloat16).astype(jnp.float32)
    return high, middle, value - high - middle


def extra_rows(rows, trio):
    row = lax.broadcasted_iota(jnp.int32, (rows, BLOCK), 0)
    values = jnp.where(row < 3, 1.0, 0.0)
    for index, value in enumerate(trio):
        values = jnp.where(row == 3 + index, value, values)
    return values.astype(jnp.bfloat16)


def column_kernel(pairs, turns, source_ref, target_ref, out_ref, peak_ref, total_ref):
    blocks, features, _ = target_ref.shape
    peak_ref[...] = jnp.full(peak_ref.shape, FLOOR, jnp.float32)
    total_ref[...] = jnp.zeros(total_ref.shape, jnp.float32)
    extra = extra_rows(LANES - features, ())

    def turn(index, carry):
        found = []
        for step in range(UNROLL):
            pair = pairs[index * UNROLL + step]
            source, target = pair >> 16, pair & 0xFFFF
            columns = target_ref[jnp.minimum(target, blocks - 1)]
            right = jnp.concatenate([columns, extra], axis=0)
            product = jnp.dot(source_ref[source], right, preferred_element_type=jnp.float32)
            product = product.reshape(BLOCK // 8, 8, BLOCK)
            peak = jnp.max(product, axis=0)
            total = jnp.sum(jnp.exp2((product - peak[None]) * exponent), axis=0)
            found.append((target, peak, total))
        for target, peak, total in found:
            old = peak_ref[target]
            new = jnp.maximum(old, peak)
            peak_ref[target] = new
            total_ref[target] = total_ref[target] * jnp.exp2(
                (old - new) * exponent
            ) + total * jnp.exp2((peak - new) * exponent)
        return carry

    lax.fori_loop(0, turns[0], turn, 0)
    peak = peak_ref[...][:blocks]
    best = jnp.max(peak, axis=1)
    out_ref[0] = best
    out_ref[1] = jnp.sum(
        total_ref[...][:blocks] * jnp.exp2((peak - best[:, None, :]) * exponent), axis=1
    )


def row_kernel(pairs, turns, source_ref, target_ref, shift_ref, out_ref, mass_ref, extra_ref):
    blocks, features, _ = target_ref.shape
    mass_ref[...] = jnp.zeros(mass_ref.shape, jnp.float32)
    width = LANES - features

    def prepare(target, carry):
        extra_ref[target] = extra_rows(width, kernel_pieces(shift_ref[pl.ds(target, 1), :]))
        return carry

    lax.fori_loop(0, blocks, prepare, 0)
    extra_ref[blocks] = extra_rows(width, (jnp.full((1, BLOCK), FLOOR, jnp.float32),))

    def turn(index, carry):
        found = []
        for step in range(UNROLL):
            pair = pairs[index * UNROLL + step]
            source, target = pair >> 16, pair & 0xFFFF
            columns = target_ref[jnp.minimum(target, blocks - 1)]
            right = jnp.concatenate([columns, extra_ref[target]], axis=0)
            product = jnp.dot(source_ref[source], right, preferred_element_type=jnp.float32)
            weights = jnp.exp2(product * exponent)
            mass_ref[source] += weights[:, :LANES] + weights[:, LANES:]
        return carry

    lax.fori_loop(0, turns[0], turn, 0)

    def finish(source, carry):
        out_ref[pl.ds(source, 1), :] = jnp.sum(mass_ref[source].T, axis=0, keepdims=True)
        return carry

    lax.fori_loop(0, out_ref.shape[0], finish, 0)


def local_call(kernel, name, out_shape, scratch, operands, count):
    vmem = pl.BlockSpec(memory_space=pltpu.VMEM)
    smem = pl.BlockSpec(memory_space=pltpu.SMEM)
    return pl.pallas_call(
        kernel,
        name=name,
        out_shape=jax.ShapeDtypeStruct(out_shape, jnp.float32),
        in_specs=[smem, smem] + [vmem] * (len(operands) - 2),
        out_specs=vmem,
        scratch_shapes=scratch,
        compiler_params=pltpu.CompilerParams(vmem_limit_bytes=28 * 2**20),
    )(*operands)


def upper_solve(upper, right_side, stored):
    values = [None] * stored
    for row in reversed(range(stored)):
        accum = right_side[row]
        for other in range(row + 1, stored):
            accum = accum - upper[row, other] * values[other]
        values[row] = accum / upper[row, row]
    return jnp.stack(values)


def lower_solve(upper, right_side, stored):
    values = [None] * stored
    for row in range(stored):
        accum = right_side[row]
        for other in range(row):
            accum = accum - upper[other, row] * values[other]
        values[row] = accum / upper[row, row]
    return jnp.stack(values)


def pair_list(block_map, counts, target_blocks, rank):
    source_blocks, listed = block_map.shape
    slots = source_blocks * listed
    padded = -(-slots // UNROLL) * UNROLL
    slot = jnp.arange(listed, dtype=jnp.int32)
    owned = (slot[None, :] < counts[:, None]) & (block_map // target_blocks == rank)
    sources = jnp.arange(source_blocks, dtype=jnp.int32)[:, None]
    packed = (sources * 65536 + block_map - rank * target_blocks).reshape(-1)
    flat = owned.reshape(-1)
    order = jnp.arange(slots, dtype=jnp.int32)
    place = jnp.sum((flat[None, :] & (order[None, :] < order[:, None])).astype(jnp.int32), axis=1)
    place = jnp.where(flat, place, -1)
    seats = jnp.arange(padded, dtype=jnp.int32)
    chosen = place[None, :] == seats[:, None]
    pairs = jnp.sum(jnp.where(chosen, packed[None, :] - target_blocks, 0), axis=1) + target_blocks
    total = jnp.sum(flat.astype(jnp.int32))
    return pairs, ((total + UNROLL - 1) // UNROLL).reshape(1)


def per_device(sources, targets, potential, block_map, counts, step_history, slope_history):
    features = sources.shape[1]
    source_blocks = potential.shape[0] // BLOCK
    target_blocks = targets.shape[0] // BLOCK
    rank = lax.axis_index("tgt")
    pairs, turns = pair_list(block_map, counts, target_blocks, rank)
    gathered = lax.all_gather(sources, "tgt", axis=0, tiled=True)
    rows = gathered.shape[0]
    extra = [piece[:, None] for piece in pieces(potential)]
    extra = jnp.concatenate(
        extra
        + [
            jnp.ones((rows, 3), jnp.float32),
            jnp.zeros((rows, LANES - features - 6), jnp.float32),
        ],
        axis=1,
    ).astype(jnp.bfloat16)
    source_tiles = jnp.concatenate([gathered, extra], axis=1).reshape(source_blocks, BLOCK, LANES)
    target_tiles = targets.reshape(target_blocks, BLOCK, features).transpose(0, 2, 1)
    state = pltpu.VMEM((target_blocks + 1, 8, BLOCK), jnp.float32)
    local = local_call(
        column_kernel,
        "columns",
        (2, target_blocks, BLOCK),
        [state, state],
        (pairs, turns, source_tiles, target_tiles),
        turns,
    )
    best = lax.pmax(local[0], "src")
    total = lax.psum(local[1] * jnp.exp2((local[0] - best) * exponent), "src")
    shift = -(best + entropy * jnp.log(total))
    target_potential = shift.reshape(-1)
    masses = local_call(
        row_kernel,
        "rows",
        (source_blocks, BLOCK),
        [
            pltpu.VMEM((source_blocks, BLOCK, LANES), jnp.float32),
            pltpu.VMEM((target_blocks + 1, LANES - features, BLOCK), jnp.bfloat16),
        ],
        (pairs, turns, source_tiles, target_tiles, shift),
        turns,
    )
    row_total = lax.psum_scatter(masses.reshape(-1), "tgt", scatter_dimension=0, tiled=True)
    ratio = source_blocks * lax.axis_size("src") / (target_blocks * lax.axis_size("tgt"))
    gradient = 1.0 - ratio * row_total
    stored = step_history.shape[0]
    highest = lax.Precision.HIGHEST
    cross_local = jnp.dot(step_history, slope_history.T, precision=highest)
    slope_local = jnp.dot(slope_history, slope_history.T, precision=highest)
    step_grad = jnp.dot(step_history, gradient, precision=highest)
    slope_grad = jnp.dot(slope_history, gradient, precision=highest)
    cross, slopes, step_dots, slope_dots = lax.psum(
        (cross_local, slope_local, step_grad, slope_grad), ("src", "tgt")
    )
    diagonal = jnp.diag(cross)
    scale = cross[stored - 1, stored - 1] / slopes[stored - 1, stored - 1]
    first_solve = upper_solve(cross, step_dots, stored)
    right_side = (
        diagonal * first_solve
        + scale * jnp.dot(slopes, first_solve, precision=highest)
        - scale * slope_dots
    )
    second_solve = lower_solve(cross, right_side, stored)
    result = (
        scale * gradient
        + jnp.dot(second_solve, step_history, precision=highest)
        - scale * jnp.dot(first_solve, slope_history, precision=highest)
    )
    direction = -result
    return (gradient, direction, target_potential)


def solution(mesh):
    in_specs = (
        P(("src", "tgt"), None),
        P("tgt", None),
        P("src"),
        P("src", None),
        P("src"),
        P(None, ("src", "tgt")),
        P(None, ("src", "tgt")),
    )
    out_specs = (P(("src", "tgt")), P(("src", "tgt")), P("tgt"))
    return jax.shard_map(
        per_device, mesh=mesh, in_specs=in_specs, out_specs=out_specs, check_vma=False
    )
```

```python
import functools
import math

import jax
import jax.numpy as jnp
from jax import lax
from jax.experimental import pallas as pl
from jax.experimental.pallas import tpu as pltpu
from jax.sharding import PartitionSpec as P

BLOCK = 256
LANES = 128
UNROLL = 4
FLOOR = -1e30

entropy = 0.5
exponent = math.log2(math.e) / entropy


def pieces(value):
    high = lax.reduce_precision(value, 8, 7)
    middle = lax.reduce_precision(value - high, 8, 7)
    low = lax.reduce_precision(value - high - middle, 8, 7)
    return high, middle, low


def kernel_pieces(value):
    high = value.astype(jnp.bfloat16).astype(jnp.float32)
    middle = (value - high).astype(jnp.bfloat16).astype(jnp.float32)
    return high, middle, value - high - middle


def extra_rows(rows, trio):
    row = lax.broadcasted_iota(jnp.int32, (rows, BLOCK), 0)
    values = jnp.where(row < 3, 1.0, 0.0)
    for index, value in enumerate(trio):
        values = jnp.where(row == 3 + index, value, values)
    return values.astype(jnp.bfloat16)


def column_kernel(pairs, turns, source_ref, target_ref, out_ref, peak_ref, total_ref):
    blocks, features, _ = target_ref.shape
    peak_ref[...] = jnp.full(peak_ref.shape, FLOOR, jnp.float32)
    total_ref[...] = jnp.zeros(total_ref.shape, jnp.float32)
    extra = extra_rows(LANES - features, ())

    def turn(index, carry):
        found = []
        for step in range(UNROLL):
            pair = pairs[index * UNROLL + step]
            source, target = pair >> 16, pair & 0xFFFF
            columns = target_ref[jnp.minimum(target, blocks - 1)]
            right = jnp.concatenate([columns, extra], axis=0)
            product = jnp.dot(source_ref[source], right, preferred_element_type=jnp.float32)
            product = product.reshape(BLOCK // 8, 8, BLOCK)
            peak = jnp.max(product, axis=0)
            total = jnp.sum(jnp.exp2((product - peak[None]) * exponent), axis=0)
            found.append((target, peak, total))
        for target, peak, total in found:
            old = peak_ref[target]
            new = jnp.maximum(old, peak)
            peak_ref[target] = new
            total_ref[target] = total_ref[target] * jnp.exp2(
                (old - new) * exponent
            ) + total * jnp.exp2((peak - new) * exponent)
        return carry

    lax.fori_loop(0, turns[0], turn, 0)
    peak = peak_ref[...][:blocks]
    best = jnp.max(peak, axis=1)
    out_ref[0] = best
    out_ref[1] = jnp.sum(
        total_ref[...][:blocks] * jnp.exp2((peak - best[:, None, :]) * exponent), axis=1
    )


def row_kernel(pairs, turns, source_ref, target_ref, shift_ref, out_ref, mass_ref, extra_ref):
    blocks, features, _ = target_ref.shape
    mass_ref[...] = jnp.zeros(mass_ref.shape, jnp.float32)
    width = LANES - features

    def prepare(target, carry):
        extra_ref[target] = extra_rows(width, kernel_pieces(shift_ref[pl.ds(target, 1), :]))
        return carry

    lax.fori_loop(0, blocks, prepare, 0)
    extra_ref[blocks] = extra_rows(width, (jnp.full((1, BLOCK), FLOOR, jnp.float32),))

    def turn(index, carry):
        found = []
        for step in range(UNROLL):
            pair = pairs[index * UNROLL + step]
            source, target = pair >> 16, pair & 0xFFFF
            columns = target_ref[jnp.minimum(target, blocks - 1)]
            right = jnp.concatenate([columns, extra_ref[target]], axis=0)
            product = jnp.dot(source_ref[source], right, preferred_element_type=jnp.float32)
            weights = jnp.exp2(product * exponent)
            mass_ref[source] += weights[:, :LANES] + weights[:, LANES:]
        return carry

    lax.fori_loop(0, turns[0], turn, 0)

    def finish(source, carry):
        out_ref[pl.ds(source, 1), :] = jnp.sum(mass_ref[source].T, axis=0, keepdims=True)
        return carry

    lax.fori_loop(0, out_ref.shape[0], finish, 0)


def local_call(kernel, name, out_shape, scratch, operands, count):
    vmem = pl.BlockSpec(memory_space=pltpu.VMEM)
    smem = pl.BlockSpec(memory_space=pltpu.SMEM)
    return pl.pallas_call(
        kernel,
        name=name,
        out_shape=jax.ShapeDtypeStruct(out_shape, jnp.float32),
        in_specs=[smem, smem] + [vmem] * (len(operands) - 2),
        out_specs=vmem,
        scratch_shapes=scratch,
        compiler_params=pltpu.CompilerParams(vmem_limit_bytes=28 * 2**20),
    )(*operands)


def exchange_kernel(axis, scatter, data_ref, out_ref, landed, send_sems, receive_sems):
    size = lax.axis_size(axis)
    me = lax.axis_index(axis)
    barrier = pltpu.get_barrier_semaphore()
    for step in range(1, size):
        pl.semaphore_signal(
            barrier,
            inc=1,
            device_id={axis: lax.rem(me + step, size)},
            device_id_type=pl.DeviceIdType.MESH,
        )
    pl.semaphore_wait(barrier, size - 1)
    copies = []
    for step in range(1, size):
        peer = lax.rem(me + step, size)
        copy = pltpu.make_async_remote_copy(
            src_ref=data_ref.at[peer] if scatter else data_ref,
            dst_ref=landed.at[step],
            send_sem=send_sems.at[step],
            recv_sem=receive_sems.at[step],
            device_id={axis: peer},
            device_id_type=pl.DeviceIdType.MESH,
        )
        copy.start()
        copies.append(copy)
    out_ref[me] = data_ref[me] if scatter else data_ref[...]
    for step in range(1, size):
        copies[step - 1].wait()
        out_ref[lax.rem(me - step + size, size)] = landed[step]


def exchange(data, axis, scatter, number):
    size = lax.axis_size(axis)
    shape = data.shape[1:] if scatter else data.shape
    vmem = pl.BlockSpec(memory_space=pltpu.VMEM)
    return pl.pallas_call(
        functools.partial(exchange_kernel, axis, scatter),
        name=f"exchange{number}",
        out_shape=jax.ShapeDtypeStruct((size,) + shape, data.dtype),
        in_specs=[vmem],
        out_specs=vmem,
        scratch_shapes=[
            pltpu.VMEM((size,) + shape, data.dtype),
            pltpu.SemaphoreType.DMA((size,)),
            pltpu.SemaphoreType.DMA((size,)),
        ],
        compiler_params=pltpu.CompilerParams(
            collective_id=number, has_side_effects=True, vmem_limit_bytes=16 * 2**20
        ),
    )(data)


def dots_kernel(step_ref, slope_ref, gradient_ref, out_ref):
    stored, points = step_ref.shape
    lane = lax.broadcasted_iota(jnp.int32, (stored, LANES), 1)
    steps, slopes = step_ref[...], slope_ref[...]
    table = jnp.zeros((stored, LANES), jnp.float32)
    others = [slope_ref[index : index + 1, :] for index in range(stored)]
    others.append(gradient_ref[...])
    for index, other in enumerate(others):
        left = jnp.sum(steps * other, axis=1, keepdims=True)
        right = jnp.sum(slopes * other, axis=1, keepdims=True)
        table = jnp.where(lane == 2 * index, left, table)
        table = jnp.where(lane == 2 * index + 1, right, table)
    out_ref[...] = table


def direction_kernel(table_ref, step_ref, slope_ref, gradient_ref, out_ref):
    stored, points = step_ref.shape
    table = jnp.sum(table_ref[...], axis=0)
    shape = (stored, LANES)
    row = lax.broadcasted_iota(jnp.int32, shape, 0)

    def column(index):
        return jnp.broadcast_to(table[:, index : index + 1], shape)

    def spread(value, index):
        return jnp.broadcast_to(value[index : index + 1, :], shape)

    cross = [column(2 * index) for index in range(stored)]
    slopes = [column(2 * index + 1) for index in range(stored)]
    step_dots, slope_dots = column(2 * stored), column(2 * stored + 1)
    scale = spread(cross[-1], stored - 1) / spread(slopes[-1], stored - 1)
    first = jnp.zeros(shape, jnp.float32)
    remains = step_dots
    product = jnp.zeros(shape, jnp.float32)
    diagonal = jnp.zeros(shape, jnp.float32)
    for index in reversed(range(stored)):
        value = spread(remains, index) / spread(cross[index], index)
        remains = remains - cross[index] * value
        first = jnp.where(row == index, value, first)
        product = product + slopes[index] * value
        diagonal = jnp.where(row == index, cross[index], diagonal)
    right_side = diagonal * first + scale * product - scale * slope_dots
    second = jnp.zeros(shape, jnp.float32)
    for index in range(stored):
        done = jnp.sum(cross[index] * second, axis=0, keepdims=True)
        value = (spread(right_side, index) - done) / spread(cross[index], index)
        second = jnp.where(row == index, value, second)
    first = scale * first
    for start in range(0, points, LANES):
        chunk = pl.ds(start, LANES)
        mixed = jnp.sum(second * step_ref[:, chunk] - first * slope_ref[:, chunk], axis=0, keepdims=True)
        out_ref[:, chunk] = -(scale[0:1, :] * gradient_ref[:, chunk] + mixed)


def plain_call(kernel, name, out_shape, operands):
    vmem = pl.BlockSpec(memory_space=pltpu.VMEM)
    return pl.pallas_call(
        kernel,
        name=name,
        out_shape=jax.ShapeDtypeStruct(out_shape, jnp.float32),
        in_specs=[vmem] * len(operands),
        out_specs=vmem,
        compiler_params=pltpu.CompilerParams(vmem_limit_bytes=16 * 2**20),
    )(*operands)


def pair_list(block_map, counts, target_blocks, rank):
    source_blocks, listed = block_map.shape
    slots = source_blocks * listed
    padded = -(-slots // UNROLL) * UNROLL
    slot = jnp.arange(listed, dtype=jnp.int32)
    owned = (slot[None, :] < counts[:, None]) & (block_map // target_blocks == rank)
    sources = jnp.arange(source_blocks, dtype=jnp.int32)[:, None]
    packed = (sources * 65536 + block_map - rank * target_blocks).reshape(-1)
    flat = owned.reshape(-1)
    order = jnp.arange(slots, dtype=jnp.int32)
    place = jnp.sum((flat[None, :] & (order[None, :] < order[:, None])).astype(jnp.int32), axis=1)
    place = jnp.where(flat, place, -1)
    seats = jnp.arange(padded, dtype=jnp.int32)
    chosen = place[None, :] == seats[:, None]
    pairs = jnp.sum(jnp.where(chosen, packed[None, :] - target_blocks, 0), axis=1) + target_blocks
    total = jnp.sum(flat.astype(jnp.int32))
    return pairs, ((total + UNROLL - 1) // UNROLL).reshape(1)


def per_device(sources, targets, potential, block_map, counts, step_history, slope_history):
    features = sources.shape[1]
    source_blocks = potential.shape[0] // BLOCK
    target_blocks = targets.shape[0] // BLOCK
    rank = lax.axis_index("tgt")
    pairs, turns = pair_list(block_map, counts, target_blocks, rank)
    gathered = lax.all_gather(sources, "tgt", axis=0, tiled=True)
    rows = gathered.shape[0]
    extra = [piece[:, None] for piece in pieces(potential)]
    extra = jnp.concatenate(
        extra
        + [
            jnp.ones((rows, 3), jnp.float32),
            jnp.zeros((rows, LANES - features - 6), jnp.float32),
        ],
        axis=1,
    ).astype(jnp.bfloat16)
    source_tiles = jnp.concatenate([gathered, extra], axis=1).reshape(source_blocks, BLOCK, LANES)
    target_tiles = targets.reshape(target_blocks, BLOCK, features).transpose(0, 2, 1)
    state = pltpu.VMEM((target_blocks + 1, 8, BLOCK), jnp.float32)
    local = local_call(
        column_kernel,
        "columns",
        (2, target_blocks, BLOCK),
        [state, state],
        (pairs, turns, source_tiles, target_tiles),
        turns,
    )
    ranks = lax.axis_size("src")
    shares = local.reshape(2, ranks, target_blocks // ranks, BLOCK).transpose(1, 0, 2, 3)
    shares = exchange(shares.reshape(ranks, -1, LANES), "src", True, 1)
    shares = shares.reshape(ranks, 2, -1, LANES)
    best = jnp.max(shares[:, 0], axis=0)
    total = jnp.sum(shares[:, 1] * jnp.exp2((shares[:, 0] - best) * exponent), axis=0)
    shift = -(best + entropy * jnp.log(total))
    shift = exchange(shift, "src", False, 2).reshape(target_blocks, BLOCK)
    target_potential = shift.reshape(-1)
    masses = local_call(
        row_kernel,
        "rows",
        (source_blocks, BLOCK),
        [
            pltpu.VMEM((source_blocks, BLOCK, LANES), jnp.float32),
            pltpu.VMEM((target_blocks + 1, LANES - features, BLOCK), jnp.bfloat16),
        ],
        (pairs, turns, source_tiles, target_tiles, shift),
        turns,
    )
    parts = exchange(masses.reshape(lax.axis_size("tgt"), -1, BLOCK), "tgt", True, 3)
    row_total = jnp.sum(parts, axis=0).reshape(1, -1)
    ratio = source_blocks * lax.axis_size("src") / (target_blocks * lax.axis_size("tgt"))
    gradient = 1.0 - ratio * row_total
    stored = step_history.shape[0]
    table = plain_call(
        dots_kernel, "dots", (stored, LANES), (step_history, slope_history, gradient)
    )
    table = jnp.sum(exchange(table, "tgt", False, 4), axis=0)
    tables = exchange(table, "src", False, 5)
    direction = plain_call(
        direction_kernel,
        "direction",
        gradient.shape,
        (tables, step_history, slope_history, gradient),
    )
    gradient, direction = gradient.reshape(-1), direction.reshape(-1)
    return (gradient, direction, target_potential)


def solution(mesh):
    in_specs = (
        P(("src", "tgt"), None),
        P("tgt", None),
        P("src"),
        P("src", None),
        P("src"),
        P(None, ("src", "tgt")),
        P(None, ("src", "tgt")),
    )
    out_specs = (P(("src", "tgt")), P(("src", "tgt")), P("tgt"))
    return jax.shard_map(
        per_device, mesh=mesh, in_specs=in_specs, out_specs=out_specs, check_vma=False
    )
```
